128 devices in a mesh: data: 1, ctx: 128 (over z, y, x, core).
Axes of the slice: x: 4, y: 4, z: 4, core: 2. Of those that a mesh axis runs over, the one named last changes fastest.
Arguments:
- hidden: bfloat16 [128, 2048], P(('data', 'ctx'))
- seq_lens: int32 [128], P(('data', 'ctx'))
- w_query: bfloat16 [16, 2048, 2048], replicated
- w_key: bfloat16 [16, 2048, 256], replicated
- w_value: bfloat16 [16, 2048, 256], replicated
- w_out: bfloat16 [16, 2048, 2048], replicated
- k_prefix: bfloat16 [16, 65536, 2, 128], P(None, ('data', 'ctx'))
- v_prefix: bfloat16 [16, 65536, 2, 128], P(None, ('data', 'ctx'))
- k_suffix: bfloat16 [16, 128, 32, 2, 128], P(None, ('data', 'ctx'))
- v_suffix: bfloat16 [16, 128, 32, 2, 128], P(None, ('data', 'ctx'))
Outputs:
- output 1: bfloat16 [128, 2048], P(('data', 'ctx'))
- output 2: bfloat16 [16, 128, 32, 2, 128], P(None, ('data', 'ctx'))
- output 3: bfloat16 [16, 128, 32, 2, 128], P(None, ('data', 'ctx'))
All inputs are finite; a program needn't handle non-finite values.
Results may differ from the reference program's by a relative error of at most 0.0135775.
Values are sent between devices in bfloat16 or wider.
A program may use at most 1.25 GiB of HBM per device.

```python
import jax
import jax.numpy as jnp
from jax import lax

MODEL_DIM = 2048
NUM_HEADS = 16
KV_HEADS = 2
HEAD_DIM = 128
LAYERS = 16
SHARDS = 128
BATCH_SIZE = 128
PREFIX_LEN = 65536
SUFFIX_LEN = 32
HOME_ROWS = 1


def setup_inputs(seed: int = 0, part: int = 0) -> dict:
    shared_keys = jax.random.split(jax.random.key(seed), 4)
    part_keys = jax.random.split(jax.random.fold_in(jax.random.key(seed + 1), part), 10)
    q_width = NUM_HEADS * HEAD_DIM
    kv_width = KV_HEADS * HEAD_DIM
    shard_rows = PREFIX_LEN // SHARDS
    w_query = jax.random.normal(shared_keys[0], (LAYERS, MODEL_DIM, q_width), jnp.float32) * MODEL_DIM ** -0.5
    w_key = jax.random.normal(shared_keys[1], (LAYERS, MODEL_DIM, kv_width), jnp.float32) * (2.5 * MODEL_DIM ** -0.5)
    w_value = jax.random.normal(shared_keys[2], (LAYERS, MODEL_DIM, kv_width), jnp.float32) * MODEL_DIM ** -0.5
    w_out = jax.random.normal(shared_keys[3], (LAYERS, q_width, MODEL_DIM), jnp.float32) * (q_width * LAYERS) ** -0.5
    hidden = jax.random.normal(part_keys[0], (BATCH_SIZE, MODEL_DIM), jnp.float32)
    centre_shape = (LAYERS, SHARDS, 1, KV_HEADS, HEAD_DIM)
    block_shape = (LAYERS, SHARDS, shard_rows, KV_HEADS, HEAD_DIM)
    prefix_shape = (LAYERS, PREFIX_LEN, KV_HEADS, HEAD_DIM)
    k_prefix = (1.5 * jax.random.normal(part_keys[1], centre_shape, jnp.float32) + jax.random.normal(part_keys[2], block_shape, jnp.float32)).reshape(prefix_shape)
    v_prefix = (jax.random.normal(part_keys[3], centre_shape, jnp.float32) + 0.5 * jax.random.normal(part_keys[4], block_shape, jnp.float32)).reshape(prefix_shape)
    seq_centre = (LAYERS, BATCH_SIZE, 1, KV_HEADS, HEAD_DIM)
    suffix_shape = (LAYERS, BATCH_SIZE, SUFFIX_LEN, KV_HEADS, HEAD_DIM)
    k_suffix = 2.5 * jax.random.normal(part_keys[5], seq_centre, jnp.float32) + jax.random.normal(part_keys[6], suffix_shape, jnp.float32)
    v_suffix = jax.random.normal(part_keys[7], seq_centre, jnp.float32) + 0.5 * jax.random.normal(part_keys[8], suffix_shape, jnp.float32)
    len_keys = jax.random.split(part_keys[9], 2)
    seq_lens = jax.random.randint(len_keys[0], (BATCH_SIZE,), 0, SUFFIX_LEN, dtype=jnp.int32)
    longest = jax.random.randint(len_keys[1], (), 0, BATCH_SIZE, dtype=jnp.int32)
    seq_lens = seq_lens.at[longest].set(SUFFIX_LEN - 1)
    seq_lens = seq_lens.at[(longest + BATCH_SIZE // 2) % BATCH_SIZE].set(0)
    return {'hidden': hidden.astype(jnp.bfloat16), 'seq_lens': seq_lens, 'w_query': w_query.astype(jnp.bfloat16), 'w_key': w_key.astype(jnp.bfloat16), 'w_value': w_value.astype(jnp.bfloat16), 'w_out': w_out.astype(jnp.bfloat16), 'k_prefix': k_prefix.astype(jnp.bfloat16), 'v_prefix': v_prefix.astype(jnp.bfloat16), 'k_suffix': k_suffix.astype(jnp.bfloat16), 'v_suffix': v_suffix.astype(jnp.bfloat16)}


def attend_block(queries, k_pre, v_pre, k_suf, v_suf, slot_live):
    score_scale = HEAD_DIM ** -0.5
    pre_scores = jnp.einsum('bkgd,pkd->bkgp', queries, k_pre) * score_scale
    suf_scores = jnp.einsum('bkgd,bskd->bkgs', queries, k_suf) * score_scale
    suf_scores = jnp.where(slot_live[:, None, None, :], suf_scores, -jnp.inf)
    row_max = jnp.maximum(pre_scores.max(axis=-1), suf_scores.max(axis=-1))
    pre_exp = jnp.exp(pre_scores - row_max[..., None])
    suf_exp = jnp.exp(suf_scores - row_max[..., None])
    mass_sum = pre_exp.sum(axis=-1) + suf_exp.sum(axis=-1)
    mixed_sum = jnp.einsum('bkgp,pkd->bkgd', pre_exp, v_pre) + jnp.einsum('bkgs,bskd->bkgd', suf_exp, v_suf)
    return mixed_sum / mass_sum[..., None]


def reference(hidden, seq_lens, w_query, w_key, w_value, w_out, k_prefix, v_prefix, k_suffix, v_suffix):
    group_size = NUM_HEADS // KV_HEADS
    blocks = BATCH_SIZE // HOME_ROWS
    slot_ids = jnp.arange(SUFFIX_LEN, dtype=jnp.int32)[None, :]
    slot_hit = (slot_ids == seq_lens[:, None])[:, :, None, None]
    slot_live = slot_ids <= seq_lens[:, None]
    live_blocks = slot_live.reshape(blocks, HOME_ROWS, SUFFIX_LEN)

    def layer_step(hidden_state, layer_args):
        q_weight, k_weight, v_weight, o_weight, k_pre, v_pre, k_suf, v_suf = layer_args
        queries = jnp.dot(hidden_state, q_weight, preferred_element_type=jnp.float32).astype(jnp.bfloat16)
        k_new = jnp.dot(hidden_state, k_weight, preferred_element_type=jnp.float32).astype(jnp.bfloat16).reshape(BATCH_SIZE, 1, KV_HEADS, HEAD_DIM)
        v_new = jnp.dot(hidden_state, v_weight, preferred_element_type=jnp.float32).astype(jnp.bfloat16).reshape(BATCH_SIZE, 1, KV_HEADS, HEAD_DIM)
        k_suf = jnp.where(slot_hit, k_new, k_suf)
        v_suf = jnp.where(slot_hit, v_new, v_suf)
        q_blocks = queries.astype(jnp.float32).reshape(blocks, HOME_ROWS, KV_HEADS, group_size, HEAD_DIM)
        k_full = k_pre.astype(jnp.float32)
        v_full = v_pre.astype(jnp.float32)
        k_blocks = k_suf.astype(jnp.float32).reshape(blocks, HOME_ROWS, SUFFIX_LEN, KV_HEADS, HEAD_DIM)
        v_blocks = v_suf.astype(jnp.float32).reshape(blocks, HOME_ROWS, SUFFIX_LEN, KV_HEADS, HEAD_DIM)
        attended = lax.map(lambda block_args: attend_block(block_args[0], k_full, v_full, block_args[1], block_args[2], block_args[3]), (q_blocks, k_blocks, v_blocks, live_blocks))
        attended = attended.astype(jnp.bfloat16).reshape(BATCH_SIZE, NUM_HEADS * HEAD_DIM)
        update = jnp.dot(attended, o_weight, preferred_element_type=jnp.float32).astype(jnp.bfloat16)
        hidden_state = (hidden_state.astype(jnp.float32) + update.astype(jnp.float32)).astype(jnp.bfloat16)
        return hidden_state, (k_suf, v_suf)

    hidden_out, cache_out = lax.scan(layer_step, hidden, (w_query, w_key, w_value, w_out, k_prefix, v_prefix, k_suffix, v_suffix))
    return hidden_out, cache_out[0], cache_out[1]
```

```python
import functools

import jax
import jax.numpy as jnp
from jax import lax
from jax.experimental import pallas as pl
from jax.experimental.pallas import tpu as pltpu
from jax.sharding import PartitionSpec as P


MESH = pl.DeviceIdType.MESH


def enter(me, count):
    barrier = pltpu.get_barrier_semaphore()

    def greet(step, carry):
        pl.semaphore_signal(barrier, inc=1, device_id={'ctx': (me + step) % count}, device_id_type=MESH)
        return carry

    lax.fori_loop(1, count, greet, 0)
    pl.semaphore_wait(barrier, count - 1)


def spread_body(count, row_ref, all_ref, send_sem, recv_sem):
    me = lax.axis_index('ctx')
    enter(me, count)

    def push(step, carry):
        pltpu.make_async_remote_copy(
            src_ref=row_ref.at[0], dst_ref=all_ref.at[me], send_sem=send_sem, recv_sem=recv_sem,
            device_id={'ctx': (me + step) % count}, device_id_type=MESH).start()
        return carry

    lax.fori_loop(1, count, push, 0)
    all_ref[me] = row_ref[0]
    others = all_ref.at[pl.ds(0, count - 1)]
    pltpu.make_async_copy(others, others, send_sem).wait()
    pltpu.make_async_copy(others, others, recv_sem).wait()


def swap_body(count, val_ref, lse_ref, vals_ref, lses_ref, send_sem, recv_sem, send_lse, recv_lse):
    me = lax.axis_index('ctx')
    enter(me, count)

    def push(step, carry):
        target = (me + step) % count
        pltpu.make_async_remote_copy(
            src_ref=val_ref.at[target], dst_ref=vals_ref.at[me], send_sem=send_sem, recv_sem=recv_sem,
            device_id={'ctx': target}, device_id_type=MESH).start()
        pltpu.make_async_remote_copy(
            src_ref=lse_ref.at[target], dst_ref=lses_ref.at[me], send_sem=send_lse, recv_sem=recv_lse,
            device_id={'ctx': target}, device_id_type=MESH).start()
        return carry

    lax.fori_loop(1, count, push, 0)
    vals_ref[me] = val_ref[me]
    lses_ref[me] = lse_ref[me]
    for block, out_sem, in_sem in ((vals_ref, send_sem, recv_sem), (lses_ref, send_lse, recv_lse)):
        others = block.at[pl.ds(0, count - 1)]
        pltpu.make_async_copy(others, others, out_sem).wait()
        pltpu.make_async_copy(others, others, in_sem).wait()


def spread(count, row):
    vmem = pl.BlockSpec(memory_space=pltpu.VMEM)
    return pl.pallas_call(
        functools.partial(spread_body, count),
        out_shape=jax.ShapeDtypeStruct((count,) + row.shape[1:], row.dtype),
        in_specs=[vmem], out_specs=vmem,
        scratch_shapes=[pltpu.SemaphoreType.DMA, pltpu.SemaphoreType.DMA],
        compiler_params=pltpu.CompilerParams(collective_id=0, has_side_effects=True),
    )(row)


def swap(count, val, lse):
    vmem = pl.BlockSpec(memory_space=pltpu.VMEM)
    return pl.pallas_call(
        functools.partial(swap_body, count),
        out_shape=(jax.ShapeDtypeStruct(val.shape, val.dtype), jax.ShapeDtypeStruct(lse.shape, lse.dtype)),
        in_specs=[vmem, vmem], out_specs=(vmem, vmem),
        scratch_shapes=[pltpu.SemaphoreType.DMA] * 4,
        compiler_params=pltpu.CompilerParams(collective_id=1, has_side_effects=True),
    )(val, lse)


def solution(mesh):
    ctx_size = mesh.shape['ctx']
    home_axes = ('data', 'ctx')
    row_spec = P(home_axes, None)
    lens_spec = P(home_axes)
    whole_spec = P()
    prefix_spec = P(None, home_axes, None, None)
    cache_spec = P(None, home_axes, None, None, None)

    def local_step(hidden, seq_lens, w_query, w_key, w_value, w_out, k_prefix, v_prefix, k_suffix, v_suffix):
        layers = w_query.shape[0]
        kv_heads = k_prefix.shape[2]
        head_dim = k_prefix.shape[3]
        num_heads = w_query.shape[2] // head_dim
        group_size = num_heads // kv_heads
        home_rows = hidden.shape[0]
        slot_count = k_suffix.shape[2]
        score_scale = head_dim ** -0.5
        slot_ids = lax.broadcasted_iota(jnp.int32, (home_rows, slot_count), 1)
        slot_hit = (slot_ids == seq_lens[:, None])[:, :, None, None]
        slot_live = (slot_ids <= seq_lens[:, None])[:, None, None, :]
        k_layers = []
        v_layers = []
        for layer_idx in range(layers):
            queries = jnp.dot(hidden, w_query[layer_idx], preferred_element_type=jnp.float32).astype(jnp.bfloat16).reshape(home_rows, kv_heads, group_size, head_dim)
            k_new = jnp.dot(hidden, w_key[layer_idx], preferred_element_type=jnp.float32).astype(jnp.bfloat16).reshape(home_rows, 1, kv_heads, head_dim)
            v_new = jnp.dot(hidden, w_value[layer_idx], preferred_element_type=jnp.float32).astype(jnp.bfloat16).reshape(home_rows, 1, kv_heads, head_dim)
            k_cache = jnp.where(slot_hit, k_new, k_suffix[layer_idx])
            v_cache = jnp.where(slot_hit, v_new, v_suffix[layer_idx])
            k_layers.append(k_cache)
            v_layers.append(v_cache)
            group_queries = spread(ctx_size, queries.reshape(home_rows, num_heads, head_dim)).reshape(ctx_size, kv_heads, group_size, head_dim)
            pre_scores = jnp.einsum('bkgd,pkd->bkgp', group_queries, k_prefix[layer_idx], preferred_element_type=jnp.float32) * score_scale
            pre_max = pre_scores.max(axis=-1)
            pre_exp = jnp.exp(pre_scores - pre_max[..., None])
            pre_mass = pre_exp.sum(axis=-1)
            pre_vals = jnp.einsum('bkgp,pkd->bkgd', pre_exp.astype(jnp.bfloat16), v_prefix[layer_idx], preferred_element_type=jnp.float32)
            part_out = (pre_vals / pre_mass[..., None]).astype(jnp.bfloat16)
            part_lse = pre_max + jnp.log(pre_mass)
            wide_lse = jnp.pad(part_lse.reshape(ctx_size, 1, num_heads), ((0, 0), (0, 0), (0, head_dim - num_heads)))
            home_out, home_lse = swap(ctx_size, part_out.reshape(ctx_size, num_heads, head_dim), wide_lse)
            home_out = home_out.reshape(ctx_size, home_rows, kv_heads, group_size, head_dim)
            home_lse = home_lse[:, 0, :num_heads].reshape(ctx_size, home_rows, kv_heads, group_size)
            suf_scores = jnp.einsum('bkgd,bskd->bkgs', queries, k_cache, preferred_element_type=jnp.float32) * score_scale
            suf_scores = jnp.where(slot_live, suf_scores, -jnp.inf)
            suf_max = suf_scores.max(axis=-1)
            suf_exp = jnp.exp(suf_scores - suf_max[..., None])
            suf_mass = suf_exp.sum(axis=-1)
            suf_vals = jnp.einsum('bkgs,bskd->bkgd', suf_exp.astype(jnp.bfloat16), v_cache, preferred_element_type=jnp.float32)
            row_max = jnp.maximum(home_lse.max(axis=0), suf_max)
            part_weight = jnp.exp(home_lse - row_max)
            suf_weight = jnp.exp(suf_max - row_max)
            mass_sum = part_weight.sum(axis=0) + suf_weight * suf_mass
            mixed_sum = (part_weight[..., None] * home_out.astype(jnp.float32)).sum(axis=0) + suf_weight[..., None] * suf_vals
            attended = (mixed_sum / mass_sum[..., None]).astype(jnp.bfloat16).reshape(home_rows, num_heads * head_dim)
            update = jnp.dot(attended, w_out[layer_idx], preferred_element_type=jnp.float32).astype(jnp.bfloat16)
            hidden = (hidden.astype(jnp.float32) + update.astype(jnp.float32)).astype(jnp.bfloat16)
        return hidden, jnp.stack(k_layers), jnp.stack(v_layers)

    return jax.shard_map(local_step, mesh=mesh, in_specs=(row_spec, lens_spec, whole_spec, whole_spec, whole_spec, whole_spec, prefix_spec, prefix_spec, cache_spec, cache_spec), out_specs=(row_spec, cache_spec, cache_spec), check_vma=False)
```
